256 devices in a mesh: groups: 4 (over x, y), blk: 64 (over z, core).
Axes of the slice: x: 2, y: 2, z: 32, core: 2. Of those that a mesh axis runs over, the one named last changes fastest.
The devices are a block of a 4x8x32 slice.
Arguments:
- snapshots: bfloat16 [4, 65536, 2, 64], P('groups', 'blk'), parts along dimension 0, may hold values from -6 to 6
- bin_index: int32 [4], P('groups'), parts along dimension 0, may hold values from 1 to 4095
- positions: int32 [3, 65536], replicated, may hold values from 0 to 511
- directions: int32 [3, 4096], replicated, may hold values from -128 to 127
- taper: float32 [65536], replicated, may hold values from 0.5 to 2
- beam_order: int32 [4096], replicated, may hold values from 0 to 4095, each once
Outputs:
- beams: bfloat16 [4096, 4, 2, 64], P('blk', 'groups'), parts along dimension 1
The draws below stay inside these ranges and needn't reach their ends.
There are 4 independent parts, one for each index of `groups`. The reference program is written for one: setup_inputs(seed, part) draws one part's arguments, and reference() takes and returns one part's arrays. A program takes and returns all parts, laid end to end along the dimension named above; an argument that names none is the same for every part. Nothing has to cross between parts.
Inputs may be any that keep to these rules, and one draw needn't show every extreme that they name: beam_order is a permutation of the 4096 beams.
All inputs are finite; a program needn't handle non-finite values.
Results may differ from the reference program's by a relative error of at most 0.0048.
Values may be sent and summed in bfloat16 or wider, within the bound.
No kernel may reach another device: no remote copies, remote signals or barrier semaphores. Data moves between devices by JAX's collectives and lax.ppermute only.
A program may use at most 64 MiB of HBM per device.

```python
import math
import jax
import jax.numpy as jnp
from jax import lax

ELEM = 65536
BEAMS = 4096
SNAP = 64
BINS = 1
CYCLE = 8192


def set_ends(entries, stream_key, low, top_value):
    shape = entries.shape
    spot = [jax.random.randint(jax.random.fold_in(stream_key, axis), (), 0, shape[axis]) for axis in range(len(shape))]
    entries = entries.at[tuple(spot)].set(low)
    longest = shape.index(max(shape))
    spot[longest] = (spot[longest] + 1) % shape[longest]
    return entries.at[tuple(spot)].set(top_value)


def block_levels(stream_key, extent, cuts, smallest, top_value):
    gain = 1.0
    for axis_at, parts in cuts:
        draws = jax.random.uniform(jax.random.fold_in(jax.random.fold_in(stream_key, 6), axis_at), (parts,), jnp.float32, smallest / len(cuts), top_value / len(cuts))
        gain = gain * jnp.repeat(jnp.exp(draws), extent[axis_at] // parts).reshape((-1,) + (1,) * (len(extent) - 1 - axis_at))
    return gain


def centred(own_key, dims, spread, most, pieces=(), held_as=jnp.bfloat16):
    drawn = spread * jax.random.normal(own_key, dims, jnp.float32)
    if pieces:
        drawn = drawn * block_levels(own_key, dims, pieces, -0.22, 0.18)
    return jnp.clip(drawn, -most, most).astype(held_as)


def setup_inputs(seed: int = 0, part: int = 0) -> dict:
    seeds = jax.random.split(jax.random.key(seed), 7)
    own_keys = jax.random.split(jax.random.fold_in(seeds[6], part), 7)
    snapshots = centred(own_keys[0], (BINS, ELEM, 2, SNAP), 1.0, 6.0, ((1, 64),))
    bin_index = jax.random.randint(own_keys[1], (BINS,), 1, CYCLE // 2).astype(jnp.int32)
    positions = set_ends(jax.random.randint(seeds[2], (3, ELEM), 0, 512), jax.random.fold_in(seeds[2], 1), 0, 511).astype(jnp.int32)
    directions = set_ends(jax.random.randint(seeds[3], (3, BEAMS), -128, 128), jax.random.fold_in(seeds[3], 1), -128, 127).astype(jnp.int32)
    taper = jnp.clip(jnp.exp(jax.random.uniform(seeds[4], (ELEM,), jnp.float32, math.log(0.5), math.log(2.0))), 0.5, 2.0)
    beam_order = jax.random.permutation(seeds[5], BEAMS).astype(jnp.int32)
    return dict(snapshots=snapshots, bin_index=bin_index, positions=positions, directions=directions, taper=taper, beam_order=beam_order)


def weight_block(dir_cols, positions, taper, bin_value):
    delays = dir_cols[0][:, None] * positions[0][None, :]
    delays = delays + dir_cols[1][:, None] * positions[1][None, :]
    delays = delays + dir_cols[2][:, None] * positions[2][None, :]
    delays = jnp.remainder(delays, CYCLE)
    phases = jnp.remainder(bin_value * delays, CYCLE)
    angles = phases.astype(jnp.float32) * (2.0 * math.pi / CYCLE)
    amplitude = (taper / math.sqrt(ELEM)).astype(jnp.float32)
    weight_re = (amplitude[None, :] * jnp.cos(angles)).astype(jnp.bfloat16)
    weight_im = (-amplitude[None, :] * jnp.sin(angles)).astype(jnp.bfloat16)
    return (weight_re, weight_im)

def beam_terms(dir_cols, positions, taper, snaps, bin_index):
    results = []
    for index in range(snaps.shape[0]):
        weight_re, weight_im = weight_block(dir_cols, positions, taper, bin_index[index])
        width = snaps.shape[3]
        columns = snaps[index].reshape(snaps.shape[1], 2 * width)
        with_real = jnp.dot(weight_re, columns, preferred_element_type=jnp.float32)
        with_imag = jnp.dot(weight_im, columns, preferred_element_type=jnp.float32)
        real_part = with_real[:, :width] - with_imag[:, width:]
        imag_part = with_real[:, width:] + with_imag[:, :width]
        results.append(jnp.stack([real_part, imag_part], axis=1))
    return jnp.stack(results, axis=1)

def reference(snapshots, bin_index, positions, directions, taper, beam_order):
    ordered = jnp.take(directions, beam_order, axis=1)
    row_block = math.gcd(BEAMS, 256)
    blocks = ordered.reshape(3, BEAMS // row_block, row_block).transpose(1, 0, 2)

    def per_block(dir_cols):
        return beam_terms(dir_cols, positions, taper, snapshots, bin_index)
    result = lax.map(per_block, blocks)
    return result.reshape(BEAMS, BINS, 2, SNAP).astype(jnp.bfloat16)
```

```python
import functools
import math

import jax
import jax.numpy as jnp
from jax import lax
from jax.experimental import pallas as pl
from jax.experimental.pallas import tpu as pltpu
from jax.sharding import PartitionSpec as P

CYCLE = 8192
CORES = 2
NEAR = 4
F32 = jnp.float32
BF16 = jnp.bfloat16
SIN = (4.442867903016298, -7.3074434206684415, 3.594788072467163, -0.7843740145897882)
COS = (-1.4142040805466873, 6.977642058572177, -5.7152384030951175, 1.7283486671441728)


def poly(coefs, z):
    total = coefs[-1]
    for coef in coefs[-2::-1]:
        total = total * z + coef
    return total


def centred(value, period):
    return ((value + period // 2) & (period - 1)) - period // 2


def beam_features(core, bin_value, dirs, order, feat, near):
    chips = order.shape[0]
    far = chips // near
    steps = centred(bin_value * dirs[...], CYCLE)
    high = (steps + 32) >> 6
    low = steps - (high << 6)
    shift = (steps[0:1] + steps[1:2] + steps[2:3]) & 31
    terms = [high.astype(F32) * (64.0 / CYCLE), low.astype(F32) * (1.0 / CYCLE), shift.astype(F32) * (256.0 / CYCLE)]
    terms = jnp.concatenate([*terms, jnp.zeros(shift.shape, F32)], axis=0)
    tiles = terms.shape[1] // 128
    table = jnp.concatenate([terms[:, 128 * q : 128 * q + 128] for q in range(tiles)], axis=0).astype(BF16)
    lane = lax.broadcasted_iota(jnp.int32, (1, 128), 1)
    sub = lax.broadcasted_iota(jnp.int32, (128, 128), 0)
    for t in range(chips // 2):
        rows = []
        for j in (2 * t, 2 * t + 1):
            chip = near * (j % far) + j // far
            rows.append(order[chip : chip + 1, :])
        first = jnp.where(core == 0, rows[0], pltpu.roll(rows[0], 64, 1))
        second = jnp.where(core == 0, pltpu.roll(rows[1], 64, 1), rows[1])
        beam = jnp.where(lane < 64, first, second)
        hot = jnp.where(sub == (beam & 127), 1.0, 0.0).astype(BF16)
        picked = jnp.dot(table, hot, preferred_element_type=F32)
        which = beam >> 7
        total = jnp.zeros((8, 128), F32)
        for q in range(tiles):
            total = jnp.where(which == q, picked[8 * q : 8 * q + 8], total)
        feat[128 * t : 128 * t + 128, :] = total.T.astype(BF16)


def weights_kernel(scal, xs0, xs1, pos0, pos1, tap0, tap1, dirs, order, out, feat, place, turned, *, near, tb, te, elem):
    beam_features(scal[1], scal[2], dirs, order, feat, near)
    parts = []
    for k, (xs, pos, tap) in enumerate(((xs0, pos0, tap0), (xs1, pos1, tap1))):
        where = (pos[...] - 256).astype(F32)
        one = jnp.ones((1, where.shape[1]), F32)
        place[k] = jnp.concatenate([where, where, one, one * 0.0], axis=0).astype(BF16)
        half = xs.shape[0] // 2
        turned[k, :half] = -xs[half:]
        turned[k, half:] = xs[:half]
        parts.append((xs, tap[...] * (1.0 / math.sqrt(elem))))
    contract = (((1,), (1,)), ((), ()))

    def step(i, carry):
        at = pl.multiple_of(i * tb, tb)
        beams = feat[pl.ds(at, tb), :]
        total = jnp.zeros((tb, out.shape[1]), F32)
        for k, (xs, amplitude) in enumerate(parts):
            for e in range(0, xs.shape[1], te):
                cols = slice(e, e + te)
                turns = jnp.dot(beams, place[k, :, cols], preferred_element_type=F32)
                r = turns - jnp.round(turns)
                z = r * r
                s = r * poly(SIN, z)
                a = amplitude[:, cols]
                scaled = a * s
                weight_re = (a - scaled * s).astype(BF16)
                weight_im = (scaled * poly(COS, z)).astype(BF16)
                total += lax.dot_general(weight_re, xs[:, cols], contract, preferred_element_type=F32)
                total += lax.dot_general(weight_im, turned[k, :, cols], contract, preferred_element_type=F32)
        out[pl.ds(at, tb), :] = total.astype(out.dtype)
        return carry

    lax.fori_loop(0, out.shape[0] // tb, step, 0)


def partial_beams(scal, mine, other, positions, taper, directions, order, near):
    cols, count = mine.shape
    elem = positions.shape[1]
    beams = directions.shape[1] // CORES
    own = lambda i, s: (0, s[0])
    mate = lambda i, s: (0, s[0] + 1 - 2 * s[1])
    whole = lambda i, s: (0, 0)
    kernel = functools.partial(weights_kernel, near=near, tb=128, te=256, elem=elem)
    return pl.pallas_call(
        kernel,
        grid_spec=pltpu.PrefetchScalarGridSpec(
            num_scalar_prefetch=1,
            grid=(1,),
            in_specs=[
                pl.BlockSpec((cols, count), whole),
                pl.BlockSpec((cols, count), whole),
                pl.BlockSpec((3, count), own),
                pl.BlockSpec((3, count), mate),
                pl.BlockSpec((1, count), own),
                pl.BlockSpec((1, count), mate),
                pl.BlockSpec(directions.shape, whole),
                pl.BlockSpec(order.shape, whole),
            ],
            out_specs=pl.BlockSpec((beams, cols), whole),
            scratch_shapes=[
                pltpu.VMEM((beams, 8), BF16),
                pltpu.VMEM((2, 8, count), BF16),
                pltpu.VMEM((2, cols, count), BF16),
            ],
        ),
        out_shape=jax.ShapeDtypeStruct((beams, cols), BF16),
        name="weights",
    )(scal, mine, other, positions, positions, taper, taper, directions, order)


def per_device(snapshots, bin_index, positions, directions, taper, beam_order):
    blocks = lax.axis_size("blk")
    chips = blocks // CORES
    far = chips // NEAR
    count = snapshots.shape[1]
    cols = snapshots.shape[2] * snapshots.shape[3]
    index = lax.axis_index("blk")
    core = index % CORES
    mine = snapshots[0].transpose(1, 2, 0).reshape(cols, count)
    other = lax.ppermute(mine, "blk", [(i, i ^ 1) for i in range(blocks)])
    scal = jnp.stack([index, core, bin_index[0]]).astype(jnp.int32)
    order = beam_order.reshape(chips, -1)
    sums = partial_beams(scal, mine, other, positions, taper[None], directions, order, NEAR)
    owned = sums.shape[0] // chips
    near_groups = [[CORES * (j * NEAR + i) + c for i in range(NEAR)] for j in range(far) for c in range(CORES)]
    far_groups = [[CORES * (i * NEAR + j) + c for i in range(far)] for j in range(NEAR) for c in range(CORES)]
    sums = sums.reshape(NEAR, far * owned, cols)
    sums = lax.all_to_all(sums, "blk", 0, 0, axis_index_groups=near_groups, tiled=True)
    sums = sums.astype(F32).sum(0).astype(BF16).reshape(far, owned, cols)
    sums = lax.all_to_all(sums, "blk", 0, 0, axis_index_groups=far_groups, tiled=True)
    sums = sums.astype(F32).sum(0).astype(BF16)
    return sums.reshape(owned, 1, snapshots.shape[2], snapshots.shape[3])


def solution(mesh):
    return jax.shard_map(
        per_device,
        mesh=mesh,
        in_specs=(P("groups", "blk", None, None), P("groups"), P(), P(), P(), P()),
        out_specs=P("blk", "groups", None, None),
        check_vma=False,
    )
```

```python
import functools
import math

import jax
import jax.numpy as jnp
from jax import lax
from jax.experimental import pallas as pl
from jax.experimental.pallas import tpu as pltpu
from jax.sharding import PartitionSpec as P

CYCLE = 8192
CORES = 2
NEAR = 4
CUTS = (4,)
TB = 1024
TE = 256
F32 = jnp.float32
BF16 = jnp.bfloat16
SIN = (4.442867903016298, -7.3074434206684415, 3.594788072467163, -0.7843740145897882)
COS = (-1.4142040805466873, 6.977642058572177, -5.7152384030951175, 1.7283486671441728)


def split_cubic(coefs):
    lead = coefs[3]
    a, b = coefs[2] / lead, coefs[1] / lead
    return lead, a, b, coefs[0] / lead - a * b


def centred(value, period):
    return ((value + period // 2) & (period - 1)) - period // 2


def beam_features(core, bin_value, dirs, order, feat, near, first, last):
    span = last - first
    steps = centred(bin_value * dirs[...], CYCLE)
    high = (steps + 32) >> 6
    low = steps - (high << 6)
    shift = (steps[0:1] + steps[1:2] + steps[2:3]) & 31
    terms = [high.astype(F32) * (64.0 / CYCLE), low.astype(F32) * (1.0 / CYCLE), shift.astype(F32) * (256.0 / CYCLE)]
    terms = jnp.concatenate([*terms, jnp.zeros(shift.shape, F32)], axis=0)
    tiles = terms.shape[1] // 128
    table = jnp.concatenate([terms[:, 128 * q : 128 * q + 128] for q in range(tiles)], axis=0).astype(BF16)
    lane = lax.broadcasted_iota(jnp.int32, (1, 128), 1)
    sub = lax.broadcasted_iota(jnp.int32, (128, 128), 0)
    for t in range(near * span // 2):
        rows = []
        for j in (2 * t, 2 * t + 1):
            chip = near * (first + j % span) + j // span
            rows.append(order[chip : chip + 1, :])
        left = jnp.where(core == 0, rows[0], pltpu.roll(rows[0], 64, 1))
        right = jnp.where(core == 0, pltpu.roll(rows[1], 64, 1), rows[1])
        beam = jnp.where(lane < 64, left, right)
        hot = jnp.where(sub == (beam & 127), 1.0, 0.0).astype(BF16)
        picked = jnp.dot(table, hot, preferred_element_type=F32)
        which = beam >> 7
        total = jnp.zeros((8, 128), F32)
        for q in range(tiles):
            total = jnp.where(which == q, picked[8 * q : 8 * q + 8], total)
        feat[128 * t : 128 * t + 128, :] = total.T.astype(BF16)


def weights_kernel(bins, mine, other, positions, taper, dirs, order, out, feat, place, turned, pos, tap, sems, *, near, first, last, tb, te):
    index = lax.axis_index("blk")
    core = index % CORES
    count = mine.shape[1]
    copies = []
    for k, owner in enumerate((index, index + 1 - 2 * core)):
        at = pl.ds(pl.multiple_of(owner * count, count), count)
        copies.append(pltpu.make_async_copy(positions.at[:, at], pos.at[k], sems.at[0, k]))
        copies.append(pltpu.make_async_copy(taper.at[:, at], tap.at[k], sems.at[1, k]))
    for copy in copies:
        copy.start()
    beam_features(core, bins[0], dirs, order, feat, near, first, last)
    for copy in copies:
        copy.wait()
    sin_lead, sin_a, sin_b, sin_c = split_cubic(SIN)
    cos_lead, cos_a, cos_b, cos_c = split_cubic(COS)
    ratio = cos_lead / sin_lead
    parts = []
    for k, xs in enumerate((mine, other)):
        where = (pos[k] - 256).astype(F32)
        one = jnp.ones((1, count), F32)
        place[k] = jnp.concatenate([where, where, one, one * 0.0], axis=0).astype(BF16)
        half = xs.shape[0] // 2
        turned[k, :half] = -xs[half:]
        turned[k, half:] = xs[:half]
        amplitude = tap[k] * (1.0 / math.sqrt(taper.shape[1]))
        parts.append((xs, amplitude, amplitude * (sin_lead * sin_lead)))
    contract = (((1,), (1,)), ((), ()))

    def step(i, carry):
        at = pl.multiple_of(i * tb, tb)
        beams = feat[pl.ds(at, tb), :]
        total = jnp.zeros((tb, out.shape[1]), F32)
        for k, (xs, amplitude, doubled) in enumerate(parts):
            for e in range(0, count, te):
                cols = slice(e, e + te)
                turns = jnp.dot(beams, place[k, :, cols], preferred_element_type=F32)
                r = turns - jnp.round(turns)
                z = r * r
                w = z * z
                t = r * ((z + sin_a) * (w + sin_b) + sin_c)
                scaled = doubled[:, cols] * t
                weight_re = (amplitude[:, cols] - scaled * t).astype(BF16)
                weight_im = (scaled * ((ratio * z + ratio * cos_a) * (w + cos_b) + ratio * cos_c)).astype(BF16)
                total += lax.dot_general(weight_re, xs[:, cols], contract, preferred_element_type=F32)
                total += lax.dot_general(weight_im, turned[k, :, cols], contract, preferred_element_type=F32)
        out[pl.ds(at, tb), :] = total.astype(out.dtype)
        return carry

    lax.fori_loop(0, out.shape[0] // tb, step, 0)


def partial_beams(bins, mine, other, positions, taper, directions, order, near, first, last):
    cols, count = mine.shape
    beams = near * (last - first) * order.shape[1] // CORES
    kernel = functools.partial(weights_kernel, near=near, first=first, last=last, tb=math.gcd(TB, beams), te=TE)
    vmem = pl.BlockSpec(memory_space=pltpu.VMEM)
    hbm = pl.BlockSpec(memory_space=pl.ANY)
    return pl.pallas_call(
        kernel,
        in_specs=[pl.BlockSpec(memory_space=pltpu.SMEM), vmem, vmem, hbm, hbm, vmem, vmem],
        out_specs=vmem,
        scratch_shapes=[
            pltpu.VMEM((beams, 8), BF16),
            pltpu.VMEM((2, 8, count), BF16),
            pltpu.VMEM((2, cols, count), BF16),
            pltpu.VMEM((2, 3, count), jnp.int32),
            pltpu.VMEM((2, 1, count), F32),
            pltpu.SemaphoreType.DMA((2, 2)),
        ],
        out_shape=jax.ShapeDtypeStruct((beams, cols), BF16),
        cost_estimate=pl.CostEstimate(flops=beams * count * cols * 8, bytes_accessed=2 * cols * count * 4, transcendentals=0),
        name=f"weights_{first}",
    )(bins, mine, other, positions, taper, directions, order)


def per_device(snapshots, bin_index, positions, directions, taper, beam_order):
    blocks = lax.axis_size("blk")
    chips = blocks // CORES
    far = chips // NEAR
    owned = beam_order.shape[0] // blocks
    count = snapshots.shape[1]
    cols = snapshots.shape[2] * snapshots.shape[3]
    mine = snapshots[0].transpose(1, 2, 0).reshape(cols, count)
    other = pltpu.with_memory_space_constraint(lax.ppermute(mine, "blk", [(i, i ^ 1) for i in range(blocks)]), pltpu.VMEM)
    order = beam_order.reshape(chips, -1)
    near_groups = [[CORES * (j * NEAR + i) + c for i in range(NEAR)] for j in range(far) for c in range(CORES)]
    far_groups = [[CORES * (i * NEAR + j) + c for i in range(far)] for j in range(NEAR) for c in range(CORES)]
    cuts = [0, *(far * c // 8 for c in CUTS), far]
    pieces = []
    for k, (first, last) in enumerate(zip(cuts[:-1], cuts[1:])):
        with jax.named_scope(f"weigh_{k}"):
            sums = partial_beams(bin_index, mine, other, positions, taper[None], directions, order, NEAR, first, last)
        with jax.named_scope(f"near_{k}"):
            sums = lax.all_to_all(sums.reshape(NEAR, -1, cols), "blk", 0, 0, axis_index_groups=near_groups, tiled=True)
        pieces.append(sums.astype(F32).sum(0).astype(BF16).reshape(last - first, owned, cols))
    sums = jnp.concatenate(pieces, axis=0)
    sums = lax.all_to_all(sums, "blk", 0, 0, axis_index_groups=far_groups, tiled=True)
    sums = sums.astype(F32).sum(0).astype(BF16)
    return sums.reshape(owned, 1, snapshots.shape[2], snapshots.shape[3])


def solution(mesh):
    return jax.shard_map(
        per_device,
        mesh=mesh,
        in_specs=(P("groups", "blk", None, None), P("groups"), P(), P(), P(), P()),
        out_specs=P("blk", "groups", None, None),
        check_vma=False,
    )
```

```python
import functools
import math

import jax
import jax.numpy as jnp
from jax import lax
from jax.experimental import pallas as pl
from jax.experimental.pallas import tpu as pltpu
from jax.sharding import PartitionSpec as P


CYCLE = 8192
CORES = 2
SHARE = 2
NEAR = 2
TB = 1024
TE = 256
F32 = jnp.float32
BF16 = jnp.bfloat16
SIN = (4.442867903016298, -7.3074434206684415, 3.594788072467163, -0.7843740145897882)
COS = (-1.4142040805466873, 6.977642058572177, -5.7152384030951175, 1.7283486671441728)


def split_cubic(coefs):
    lead = coefs[3]
    a, b = coefs[2] / lead, coefs[1] / lead
    return lead, a, b, coefs[0] / lead - a * b


def centred(value, period):
    return ((value + period // 2) & (period - 1)) - period // 2


def beam_features(chip, core, bin_value, dirs, order, feat, near, share):
    chips = order.shape[0]
    far = chips // (near * share)
    steps = centred(bin_value * dirs[...], CYCLE)
    high = (steps + 32) >> 6
    low = steps - (high << 6)
    shift = (steps[0:1] + steps[1:2] + steps[2:3]) & 31
    terms = [high.astype(F32) * (64.0 / CYCLE), low.astype(F32) * (1.0 / CYCLE), shift.astype(F32) * (256.0 / CYCLE)]
    terms = jnp.concatenate([*terms, jnp.zeros(shift.shape, F32)], axis=0)
    tiles = terms.shape[1] // 128
    table = jnp.concatenate([terms[:, 128 * q : 128 * q + 128] for q in range(tiles)], axis=0).astype(BF16)
    lane = lax.broadcasted_iota(jnp.int32, (1, 128), 1)
    sub = lax.broadcasted_iota(jnp.int32, (128, 128), 0)
    for t in range(near * far // 2):
        rows = []
        for j in (2 * t, 2 * t + 1):
            side = (chip // share + 1 + j // far) % near
            owner = share * (near * (j % far) + side) + chip % share
            rows.append(order[pl.ds(owner, 1), :])
        left = jnp.where(core == 0, rows[0], pltpu.roll(rows[0], 64, 1))
        right = jnp.where(core == 0, pltpu.roll(rows[1], 64, 1), rows[1])
        beam = jnp.where(lane < 64, left, right)
        hot = jnp.where(sub == (beam & 127), 1.0, 0.0).astype(BF16)
        picked = jnp.dot(table, hot, preferred_element_type=F32)
        which = beam >> 7
        total = jnp.zeros((8, 128), F32)
        for q in range(tiles):
            total = jnp.where(which == q, picked[8 * q : 8 * q + 8], total)
        feat[128 * t : 128 * t + 128, :] = total.T.astype(BF16)


def weights_kernel(*refs, near, share, flip, row, tb, te):
    first = flip == 0
    if first:
        bins, mine, other, positions, taper, dirs, order, out, feat, place, turned, pos, tap, sems = refs
    else:
        mine, other, positions, taper, feat, start, out, place, turned, pos, tap, sems = refs
    index = lax.axis_index("blk")
    core = index % CORES
    chip = index // CORES
    source = chip + flip * (1 - 2 * (chip % share))
    count = mine.shape[1]
    copies = []
    for k, owner in enumerate((CORES * source + core, CORES * source + 1 - core)):
        at = pl.ds(pl.multiple_of(owner * count, count), count)
        copies.append(pltpu.make_async_copy(positions.at[:, at], pos.at[k], sems.at[0, k]))
        copies.append(pltpu.make_async_copy(taper.at[:, at], tap.at[k], sems.at[1, k]))
    for copy in copies:
        copy.start()
    if first:
        beam_features(chip, core, bins[0], dirs, order, feat, near, share)
    for copy in copies:
        copy.wait()
    sin_lead, sin_a, sin_b, sin_c = split_cubic(SIN)
    cos_lead, cos_a, cos_b, cos_c = split_cubic(COS)
    ratio = cos_lead / sin_lead
    parts = []
    for k, xs in enumerate((mine, other)):
        where = (pos[k] - 256).astype(F32)
        one = jnp.ones((1, count), F32)
        place[k] = jnp.concatenate([where, where, one, one * 0.0], axis=0).astype(BF16)
        half = xs.shape[0] // 2
        turned[k, :half] = -xs[half:]
        turned[k, half:] = xs[:half]
        amplitude = tap[k] * (1.0 / math.sqrt(taper.shape[1]))
        parts.append((xs, amplitude, amplitude * (sin_lead * sin_lead)))
    contract = (((1,), (1,)), ((), ()))

    def step(i, carry):
        at = pl.multiple_of(i * tb, tb)
        beams = feat[pl.ds(row + at, tb), :]
        total = jnp.zeros((tb, out.shape[1]), F32)
        for k, (xs, amplitude, doubled) in enumerate(parts):
            for e in range(0, count, te):
                cols = slice(e, e + te)
                turns = jnp.dot(beams, place[k, :, cols], preferred_element_type=F32)
                r = turns - jnp.round(turns)
                z = r * r
                w = z * z
                t = r * ((z + sin_a) * (w + sin_b) + sin_c)
                scaled = doubled[:, cols] * t
                weight_re = (amplitude[:, cols] - scaled * t).astype(BF16)
                weight_im = (scaled * ((ratio * z + ratio * cos_a) * (w + cos_b) + ratio * cos_c)).astype(BF16)
                total += lax.dot_general(weight_re, xs[:, cols], contract, preferred_element_type=F32)
                total += lax.dot_general(weight_im, turned[k, :, cols], contract, preferred_element_type=F32)
        if not first:
            total += start[pl.ds(row + at, tb), :]
        out[pl.ds(at, tb), :] = total.astype(out.dtype)
        return carry

    lax.fori_loop(0, out.shape[0] // tb, step, 0)


def partial_beams(flip, operands, near, share, row, beams, kind):
    cols, count = operands[1 - flip].shape
    kernel = functools.partial(weights_kernel, near=near, share=share, flip=flip, row=row, tb=math.gcd(TB, beams), te=TE)
    vmem = pl.BlockSpec(memory_space=pltpu.VMEM)
    hbm = pl.BlockSpec(memory_space=pl.ANY)
    if flip:
        in_specs = [vmem, vmem, hbm, hbm, vmem, vmem]
        out_shape = pltpu.VMEM((beams, cols), kind)
    else:
        in_specs = [pl.BlockSpec(memory_space=pltpu.SMEM), vmem, vmem, hbm, hbm, vmem, vmem]
        out_shape = (pltpu.VMEM((beams, cols), kind), pltpu.VMEM((beams, 8), BF16))
    return pl.pallas_call(
        kernel,
        in_specs=in_specs,
        out_specs=vmem if flip else (vmem, vmem),
        scratch_shapes=[
            pltpu.VMEM((2, 8, count), BF16),
            pltpu.VMEM((2, cols, count), BF16),
            pltpu.VMEM((2, 3, count), jnp.int32),
            pltpu.VMEM((2, 1, count), F32),
            pltpu.SemaphoreType.DMA((2, 2)),
        ],
        out_shape=out_shape,
        cost_estimate=pl.CostEstimate(flops=beams * count * cols * 8, bytes_accessed=2 * cols * count * 4, transcendentals=0),
    )(*operands)


def per_device(snapshots, bin_index, positions, directions, taper, beam_order):
    blocks = lax.axis_size("blk")
    chips = blocks // CORES
    side = SHARE * NEAR
    far = chips // side
    owned = beam_order.shape[0] // blocks
    count = snapshots.shape[1]
    cols = snapshots.shape[2] * snapshots.shape[3]
    beams = beam_order.shape[0] // (CORES * SHARE)

    def swap(value, bit):
        return lax.ppermute(value, "blk", [(i, i ^ bit) for i in range(blocks)])

    def near_by(*values):
        return [pltpu.with_memory_space_constraint(value, pltpu.VMEM) for value in values]

    mine = snapshots[0].transpose(1, 2, 0).reshape(cols, count)
    other = swap(mine, 1)
    across = swap(mine, CORES)
    order = beam_order.reshape(chips, -1)
    (other,) = near_by(other)
    sums, feat = partial_beams(0, (bin_index, mine, other, positions, taper[None], directions, order), NEAR, SHARE, 0, beams, F32)
    across, sums = lax.optimization_barrier((across, sums))
    across_other = swap(across, 1)
    across, across_other, feat, sums = near_by(across, across_other, feat, sums)
    operands = (across, across_other, positions, taper[None], feat, sums)
    half = beams // NEAR
    given = partial_beams(1, operands, NEAR, SHARE, 0, half, BF16)
    given = swap(given, CORES * SHARE)
    kept = partial_beams(1, operands, NEAR, SHARE, half, half, F32)
    sums = (kept + given.astype(F32)).astype(BF16).reshape(far, owned, cols)
    far_groups = [[CORES * (i * side + j) + c for i in range(far)] for j in range(side) for c in range(CORES)]
    sums = lax.all_to_all(sums, "blk", 0, 0, axis_index_groups=far_groups, tiled=True)
    sums = sums.astype(F32).sum(0).astype(BF16)
    return sums.reshape(owned, 1, snapshots.shape[2], snapshots.shape[3])


def solution(mesh):
    return jax.shard_map(
        per_device,
        mesh=mesh,
        in_specs=(P("groups", "blk", None, None), P("groups"), P(), P(), P(), P()),
        out_specs=P("blk", "groups", None, None),
        check_vma=False,
    )
```

```python
import functools
import math

import jax
import jax.numpy as jnp
from jax import lax
from jax.experimental import pallas as pl
from jax.experimental.pallas import tpu as pltpu
from jax.sharding import PartitionSpec as P


CYCLE = 8192
CORES = 2
SHARE = 2
TB = 512
TE = 256
F32 = jnp.float32
BF16 = jnp.bfloat16
SIN = (4.442867903016298, -7.3074434206684415, 3.594788072467163, -0.7843740145897882)
COS = (-1.4142040805466873, 6.977642058572177, -5.7152384030951175, 1.7283486671441728)


def split_cubic(coefs):
    lead = coefs[3]
    a, b = coefs[2] / lead, coefs[1] / lead
    return lead, a, b, coefs[0] / lead - a * b


def centred(value, period):
    return ((value + period // 2) & (period - 1)) - period // 2


def owner_of(j, chip, chips, share):
    side = 2 * share
    far = chips // side
    near = (chip ^ share) if j < far else chip
    return side * (j % far) + near % side


def beam_features(chip, core, bin_value, dirs, order, feat, share):
    chips = order.shape[0]
    steps = centred(bin_value * dirs[...], CYCLE)
    high = (steps + 32) >> 6
    low = steps - (high << 6)
    shift = (steps[0:1] + steps[1:2] + steps[2:3]) & 31
    terms = [high.astype(F32) * (64.0 / CYCLE), low.astype(F32) * (1.0 / CYCLE), shift.astype(F32) * (256.0 / CYCLE)]
    terms = jnp.concatenate([*terms, jnp.zeros(shift.shape, F32)], axis=0)
    tiles = terms.shape[1] // 128
    table = jnp.concatenate([terms[:, 128 * q : 128 * q + 128] for q in range(tiles)], axis=0).astype(BF16)
    lane = lax.broadcasted_iota(jnp.int32, (1, 128), 1)
    sub = lax.broadcasted_iota(jnp.int32, (128, 128), 0)
    for t in range(chips // share // 2):
        rows = []
        for j in (2 * t, 2 * t + 1):
            owner = owner_of(j, chip, chips, share)
            rows.append(order[pl.ds(owner, 1), :])
        left = jnp.where(core == 0, rows[0], pltpu.roll(rows[0], 64, 1))
        right = jnp.where(core == 0, pltpu.roll(rows[1], 64, 1), rows[1])
        beam = jnp.where(lane < 64, left, right)
        hot = jnp.where(sub == (beam & 127), 1.0, 0.0).astype(BF16)
        picked = jnp.dot(table, hot, preferred_element_type=F32)
        which = beam >> 7
        total = jnp.zeros((8, 128), F32)
        for q in range(tiles):
            total = jnp.where(which == q, picked[8 * q : 8 * q + 8], total)
        feat[128 * t : 128 * t + 128, :] = total.T.astype(BF16)


def element_features(index, positions, taper, place, shade, pos, sems):
    parts, _, count = pos.shape
    copies = []
    for k in range(parts):
        at = pl.ds(pl.multiple_of((index ^ k) * count, count), count)
        copies.append(pltpu.make_async_copy(positions.at[:, at], pos.at[k], sems.at[0, k]))
        copies.append(pltpu.make_async_copy(taper.at[:, at], shade.at[k], sems.at[1, k]))
    for copy in copies:
        copy.start()
    yield
    for copy in copies:
        copy.wait()
    one = jnp.ones((1, count), F32)
    for k in range(parts):
        where = (pos[k] - 256).astype(F32)
        place[k] = jnp.concatenate([where, where, one, one * 0.0], axis=0).astype(BF16)
        shade[k] = shade[k] * (1.0 / math.sqrt(taper.shape[1]))


def weigh(xs_refs, pieces, feat, place, shade, turned, start, out, row, tb, te):
    count = place.shape[2]
    sin_lead, sin_a, sin_b, sin_c = split_cubic(SIN)
    cos_lead, cos_a, cos_b, cos_c = split_cubic(COS)
    ratio = cos_lead / sin_lead
    parts = []
    for slot, (xs, k) in enumerate(zip(xs_refs, pieces)):
        half = xs.shape[0] // 2
        turned[slot, :half] = -xs[half:]
        turned[slot, half:] = xs[:half]
        amplitude = shade[k]
        parts.append((xs, k, slot, amplitude, amplitude * (sin_lead * sin_lead)))
    contract = (((1,), (1,)), ((), ()))

    def step(i, carry):
        at = pl.multiple_of(i * tb, tb)
        beams = feat[pl.ds(row + at, tb), :]
        total = jnp.zeros((tb, out.shape[1]), F32) if start is None else start[pl.ds(at, tb), :]
        for xs, k, slot, amplitude, doubled in parts:
            for e in range(0, count, te):
                cols = slice(e, e + te)
                turns = jnp.dot(beams, place[k, :, cols], preferred_element_type=F32)
                r = turns - jnp.round(turns)
                z = r * r
                w = z * z
                t = r * ((z + sin_a) * (w + sin_b) + sin_c)
                scaled = doubled[:, cols] * t
                weight_re = (amplitude[:, cols] - scaled * t).astype(BF16)
                weight_im = (scaled * ((ratio * z + ratio * cos_a) * (w + cos_b) + ratio * cos_c)).astype(BF16)
                total += lax.dot_general(weight_re, xs[:, cols], contract, preferred_element_type=F32)
                total += lax.dot_general(weight_im, turned[slot, :, cols], contract, preferred_element_type=F32)
        out[pl.ds(at, tb), :] = total.astype(out.dtype)
        return carry

    lax.fori_loop(0, out.shape[0] // tb, step, 0)


def first_kernel(bins, mine, other, positions, taper, dirs, order, out, feat, place, shade, turned, pos, sems, *, share, tb, te):
    index = lax.axis_index("blk")
    elements = element_features(index, positions, taper, place, shade, pos, sems)
    next(elements)
    beam_features(index // CORES, index % CORES, bins[0], dirs, order, feat, share)
    next(elements, None)
    weigh((mine, other), (0, 1), feat, place, shade, turned, None, out, 0, tb, te)


def given_kernel(xs, feat, place, shade, start, out, turned, *, piece, tb, te):
    weigh((xs,), (piece,), feat, place, shade, turned, start, out, 0, tb, te)


def kept_kernel(mine, other, across, across_other, feat, place, shade, out, turned, *, row, tb, te):
    weigh((mine, other, across, across_other), (0, 1, 2, 3), feat, place, shade, turned, None, out, row, tb, te)


def per_device(snapshots, bin_index, positions, directions, taper, beam_order):
    blocks = lax.axis_size("blk")
    chips = blocks // CORES
    parts = CORES * SHARE
    count = snapshots.shape[1]
    cols = snapshots.shape[2] * snapshots.shape[3]
    beams = beam_order.shape[0] // parts
    half = beams // 2
    vmem = pl.BlockSpec(memory_space=pltpu.VMEM)
    hbm = pl.BlockSpec(memory_space=pl.ANY)

    def swap(value, bit):
        return lax.ppermute(value, "blk", [(i, i ^ bit) for i in range(blocks)])

    def near_by(*values):
        return [pltpu.with_memory_space_constraint(value, pltpu.VMEM) for value in values]

    def call(kernel, in_specs, out_shape, scratch, operands, slots):
        return pl.pallas_call(
            kernel,
            in_specs=in_specs,
            out_specs=jax.tree.map(lambda _: vmem, out_shape),
            out_shape=out_shape,
            scratch_shapes=[pltpu.VMEM((slots, cols, count), BF16), *scratch],
            cost_estimate=pl.CostEstimate(flops=half * slots * count * cols * 8, bytes_accessed=2 * cols * count * 4, transcendentals=0),
        )(*operands)

    mine = snapshots[0].transpose(1, 2, 0).reshape(cols, count)
    other = swap(mine, 1)
    across = swap(mine, CORES)
    order = beam_order.reshape(chips, -1)
    (other,) = near_by(other)
    sums, feat, place, shade = call(
        functools.partial(first_kernel, share=SHARE, tb=math.gcd(TB, half), te=TE),
        [pl.BlockSpec(memory_space=pltpu.SMEM), vmem, vmem, hbm, hbm, vmem, vmem],
        (
            pltpu.VMEM((half, cols), F32),
            pltpu.VMEM((beams, 8), BF16),
            pltpu.VMEM((parts, 8, count), BF16),
            pltpu.VMEM((parts, 1, count), F32),
        ),
        [pltpu.VMEM((parts, 3, count), jnp.int32), pltpu.SemaphoreType.DMA((2, parts))],
        (bin_index, mine, other, positions, taper[None], directions, order),
        2,
    )
    across, sums = lax.optimization_barrier((across, sums))
    across_other = swap(across, 1)
    across, across_other, feat, place, shade, sums = near_by(across, across_other, feat, place, shade, sums)

    def give(xs, piece, start, kind):
        return call(
            functools.partial(given_kernel, piece=piece, tb=math.gcd(TB, half), te=TE),
            [vmem] * 5,
            pltpu.VMEM((half, cols), kind),
            [],
            (xs, feat, place, shade, start),
            1,
        )

    (sums,) = near_by(give(across, 2, sums, F32))
    given = give(across_other, 3, sums, BF16)
    given = swap(given, CORES * SHARE)
    kept = call(
        functools.partial(kept_kernel, row=half, tb=math.gcd(TB, half), te=TE),
        [vmem] * 7,
        pltpu.VMEM((half, cols), F32),
        [],
        (*near_by(mine), other, across, across_other, feat, place, shade),
        4,
    )
    sums = kept + given.astype(F32)
    side = SHARE * 2
    far = chips // side
    far_groups = [[CORES * (i * side + j) + c for i in range(far)] for j in range(side) for c in range(CORES)]
    sums = sums.astype(BF16).reshape(far, -1, cols)
    sums = lax.all_to_all(sums, "blk", 0, 0, axis_index_groups=far_groups, tiled=True)
    sums = sums.astype(F32).sum(0).astype(BF16)
    return sums.reshape(-1, 1, snapshots.shape[2], snapshots.shape[3])


def solution(mesh):
    return jax.shard_map(
        per_device,
        mesh=mesh,
        in_specs=(P("groups", "blk", None, None), P("groups"), P(), P(), P(), P()),
        out_specs=P("blk", "groups", None, None),
        check_vma=False,
    )
```

```python
import functools
import math

import jax
import jax.numpy as jnp
from jax import lax
from jax.experimental import pallas as pl
from jax.experimental.pallas import tpu as pltpu
from jax.sharding import PartitionSpec as P


CYCLE = 8192
CORES = 2
SHARE = 2
HOPS = (-2, 1, 4, -1, 2, -3, 0, 3)
TB = 512
TE = 256
F32 = jnp.float32
BF16 = jnp.bfloat16
SIN = (4.442867903016298, -7.3074434206684415, 3.594788072467163, -0.7843740145897882)
COS = (-1.4142040805466873, 6.977642058572177, -5.7152384030951175, 1.7283486671441728)


def split_cubic(coefs):
    lead = coefs[3]
    a, b = coefs[2] / lead, coefs[1] / lead
    return lead, a, b, coefs[0] / lead - a * b


def centred(value, period):
    return ((value + period // 2) & (period - 1)) - period // 2


def owner_of(j, chip, chips, share):
    side = 2 * share
    far = chips // side
    near = (chip ^ share) if j < far else chip
    return side * ((chip // side + HOPS[j % far]) % far) + near % side


def beam_features(chip, core, bin_value, dirs, order, feat, share):
    chips = order.shape[0]
    steps = centred(bin_value * dirs[...], CYCLE)
    high = (steps + 32) >> 6
    low = steps - (high << 6)
    shift = (steps[0:1] + steps[1:2] + steps[2:3]) & 31
    terms = [high.astype(F32) * (64.0 / CYCLE), low.astype(F32) * (1.0 / CYCLE), shift.astype(F32) * (256.0 / CYCLE)]
    terms = jnp.concatenate([*terms, jnp.zeros(shift.shape, F32)], axis=0)
    tiles = terms.shape[1] // 128
    table = jnp.concatenate([terms[:, 128 * q : 128 * q + 128] for q in range(tiles)], axis=0).astype(BF16)
    lane = lax.broadcasted_iota(jnp.int32, (1, 128), 1)
    sub = lax.broadcasted_iota(jnp.int32, (128, 128), 0)
    for t in range(chips // share // 2):
        rows = []
        for j in (2 * t, 2 * t + 1):
            owner = owner_of(j, chip, chips, share)
            rows.append(order[pl.ds(owner, 1), :])
        left = jnp.where(core == 0, rows[0], pltpu.roll(rows[0], 64, 1))
        right = jnp.where(core == 0, pltpu.roll(rows[1], 64, 1), rows[1])
        beam = jnp.where(lane < 64, left, right)
        hot = jnp.where(sub == (beam & 127), 1.0, 0.0).astype(BF16)
        picked = jnp.dot(table, hot, preferred_element_type=F32)
        which = beam >> 7
        total = jnp.zeros((8, 128), F32)
        for q in range(tiles):
            total = jnp.where(which == q, picked[8 * q : 8 * q + 8], total)
        feat[128 * t : 128 * t + 128, :] = total.T.astype(BF16)


def element_features(index, positions, taper, place, shade, pos, sems):
    parts, _, count = pos.shape
    copies = []
    for k in range(parts):
        at = pl.ds(pl.multiple_of((index ^ k) * count, count), count)
        copies.append(pltpu.make_async_copy(positions.at[:, at], pos.at[k], sems.at[0, k]))
        copies.append(pltpu.make_async_copy(taper.at[:, at], shade.at[k], sems.at[1, k]))
    for copy in copies:
        copy.start()
    yield
    for copy in copies:
        copy.wait()
    one = jnp.ones((1, count), F32)
    for k in range(parts):
        where = (pos[k] - 256).astype(F32)
        place[k] = jnp.concatenate([where, where, one, one * 0.0], axis=0).astype(BF16)
        shade[k] = shade[k] * (1.0 / math.sqrt(taper.shape[1]))


def weigh(xs_refs, pieces, feat, place, shade, turned, start, out, row, tb, te):
    count = place.shape[2]
    sin_lead, sin_a, sin_b, sin_c = split_cubic(SIN)
    cos_lead, cos_a, cos_b, cos_c = split_cubic(COS)
    ratio = cos_lead / sin_lead
    parts = []
    for slot, (xs, k) in enumerate(zip(xs_refs, pieces)):
        half = xs.shape[0] // 2
        turned[slot, :half] = -xs[half:]
        turned[slot, half:] = xs[:half]
        amplitude = shade[k]
        parts.append((xs, k, slot, amplitude, amplitude * (sin_lead * sin_lead)))
    contract = (((1,), (1,)), ((), ()))

    def step(i, carry):
        at = pl.multiple_of(i * tb, tb)
        beams = feat[pl.ds(row + at, tb), :]
        total = jnp.zeros((tb, out.shape[1]), F32) if start is None else start[pl.ds(at, tb), :]
        for xs, k, slot, amplitude, doubled in parts:
            for e in range(0, count, te):
                cols = slice(e, e + te)
                turns = jnp.dot(beams, place[k, :, cols], preferred_element_type=F32)
                r = turns - jnp.round(turns)
                z = r * r
                w = z * z
                t = r * ((z + sin_a) * (w + sin_b) + sin_c)
                scaled = doubled[:, cols] * t
                weight_re = (amplitude[:, cols] - scaled * t).astype(BF16)
                weight_im = (scaled * ((ratio * z + ratio * cos_a) * (w + cos_b) + ratio * cos_c)).astype(BF16)
                total += lax.dot_general(weight_re, xs[:, cols], contract, preferred_element_type=F32)
                total += lax.dot_general(weight_im, turned[slot, :, cols], contract, preferred_element_type=F32)
        out[pl.ds(at, tb), :] = total.astype(out.dtype)
        return carry

    lax.fori_loop(0, out.shape[0] // tb, step, 0)


def first_kernel(bins, mine, other, positions, taper, dirs, order, out, feat, place, shade, turned, pos, sems, *, share, tb, te):
    index = lax.axis_index("blk")
    elements = element_features(index, positions, taper, place, shade, pos, sems)
    next(elements)
    beam_features(index // CORES, index % CORES, bins[0], dirs, order, feat, share)
    next(elements, None)
    weigh((mine, other), (0, 1), feat, place, shade, turned, None, out, 0, tb, te)


def given_kernel(xs, feat, place, shade, start, out, turned, *, piece, tb, te):
    weigh((xs,), (piece,), feat, place, shade, turned, start, out, 0, tb, te)


def kept_kernel(mine, other, across, across_other, feat, place, shade, out, turned, *, row, tb, te):
    weigh((mine, other, across, across_other), (0, 1, 2, 3), feat, place, shade, turned, None, out, row, tb, te)


def per_device(snapshots, bin_index, positions, directions, taper, beam_order):
    blocks = lax.axis_size("blk")
    chips = blocks // CORES
    parts = CORES * SHARE
    count = snapshots.shape[1]
    cols = snapshots.shape[2] * snapshots.shape[3]
    beams = beam_order.shape[0] // parts
    half = beams // 2
    vmem = pl.BlockSpec(memory_space=pltpu.VMEM)
    hbm = pl.BlockSpec(memory_space=pl.ANY)

    def swap(value, bit):
        return lax.ppermute(value, "blk", [(i, i ^ bit) for i in range(blocks)])

    def near_by(*values):
        return [pltpu.with_memory_space_constraint(value, pltpu.VMEM) for value in values]

    def call(kernel, in_specs, out_shape, scratch, operands, slots):
        return pl.pallas_call(
            kernel,
            in_specs=in_specs,
            out_specs=jax.tree.map(lambda _: vmem, out_shape),
            out_shape=out_shape,
            scratch_shapes=[pltpu.VMEM((slots, cols, count), BF16), *scratch],
            cost_estimate=pl.CostEstimate(flops=half * slots * count * cols * 8, bytes_accessed=2 * cols * count * 4, transcendentals=0),
        )(*operands)

    mine = snapshots[0].transpose(1, 2, 0).reshape(cols, count)
    other = swap(mine, 1)
    across = swap(mine, CORES)
    order = beam_order.reshape(chips, -1)
    (other,) = near_by(other)
    sums, feat, place, shade = call(
        functools.partial(first_kernel, share=SHARE, tb=math.gcd(TB, half), te=TE),
        [pl.BlockSpec(memory_space=pltpu.SMEM), vmem, vmem, hbm, hbm, vmem, vmem],
        (
            pltpu.VMEM((half, cols), F32),
            pltpu.VMEM((beams, 8), BF16),
            pltpu.VMEM((parts, 8, count), BF16),
            pltpu.VMEM((parts, 1, count), F32),
        ),
        [pltpu.VMEM((parts, 3, count), jnp.int32), pltpu.SemaphoreType.DMA((2, parts))],
        (bin_index, mine, other, positions, taper[None], directions, order),
        2,
    )
    across, sums = lax.optimization_barrier((across, sums))
    across_other = swap(across, 1)
    across, across_other, feat, place, shade, sums = near_by(across, across_other, feat, place, shade, sums)

    def give(xs, piece, start, kind):
        return call(
            functools.partial(given_kernel, piece=piece, tb=math.gcd(TB, half), te=TE),
            [vmem] * 5,
            pltpu.VMEM((half, cols), kind),
            [],
            (xs, feat, place, shade, start),
            1,
        )

    (sums,) = near_by(give(across, 2, sums, F32))
    given = give(across_other, 3, sums, BF16)
    given = swap(given, CORES * SHARE)
    kept = call(
        functools.partial(kept_kernel, row=half, tb=math.gcd(TB, half), te=TE),
        [vmem] * 7,
        pltpu.VMEM((half, cols), F32),
        [],
        (*near_by(mine), other, across, across_other, feat, place, shade),
        4,
    )
    sums = kept + given.astype(F32)
    side = CORES * SHARE * 2
    rows = half // len(HOPS)

    def shift(value, far):
        return lax.ppermute(value.astype(BF16), "blk", [(i, (i + far * side) % blocks) for i in range(blocks)]).astype(F32)

    up = shift(sums[: 3 * rows], 1)
    down = shift(sums[3 * rows : 5 * rows], -1)
    sums = sums[5 * rows :] + up
    below, own, above = sums[:rows], sums[rows : 2 * rows] + down[:rows], sums[2 * rows :] + down[rows:]
    sums = own + shift(above, 3) + shift(below, -3)
    return sums.astype(BF16).reshape(-1, 1, snapshots.shape[2], snapshots.shape[3])


def solution(mesh):
    return jax.shard_map(
        per_device,
        mesh=mesh,
        in_specs=(P("groups", "blk", None, None), P("groups"), P(), P(), P(), P()),
        out_specs=P("blk", "groups", None, None),
        check_vma=False,
    )
```
